32 devices in a mesh: grp: 4 (over y, x), dev: 8 (over z, core).
Axes of the slice: x: 2, y: 2, z: 4, core: 2. Of those that a mesh axis runs over, the one named last changes fastest.
Arguments:
- obs_coord: float32 [3, 131072], P(None, ('grp', 'dev')), may hold values from -1 to 1
- obs_resid: float32 [131072], P(('grp', 'dev')), may hold values from -6 to 6
- obs_weight: float32 [131072], P(('grp', 'dev')), may hold values from 0.5 to 2
- obs_dest: int32 [131072], P(('grp', 'dev')), may hold values from 0 to 7, as said below
- obs_send_slot: int32 [131072], P(('grp', 'dev')), may hold values from 0 to 1023, as said below
- obs_elem: int32 [131072], P(('grp', 'dev')), may hold values from 0 to 255, as said below
- obs_slot: int32 [131072], P(('grp', 'dev')), may hold values from 0 to 31, as said below
Outputs:
- nodal: float32 [16, 64, 8, 512], P('grp', 'dev')
- total_cost: float32 [], replicated
The draws below stay inside these ranges and needn't reach their ends.
Inputs may be any that keep to these rules, and one draw needn't show every extreme that they name: `obs_dest`: from the rows of one device, at most 1024 observations go to any one destination; in every group one destination receives exactly 1024 from every device of the group. `obs_send_slot`: distinct among the rows of one device with the same obs_dest. `obs_elem`: together with obs_slot distinct among all observations of a group with the same obs_dest. `obs_slot`: on every destination some element uses all 32 slots.
All inputs are finite; a program needn't handle non-finite values.
Results may differ from the reference program's by a relative error of at most 0.00017.
Values sent between devices are 32-bit elements; how exact they have to be, the bound alone decides.
No kernel may reach another device: no remote copies, remote signals or barrier semaphores. Data moves between devices by JAX's collectives and lax.ppermute only.
A program may use at most 64 MiB of HBM per device.

```python
import math
import jax
import jax.numpy as jnp
from jax import lax

OBS_DEV = 4096
EX = 4
EY = 8
EZ = 8
ELEM_DEV = 256
CAP = 1024
SLOTS = 32
TOTAL_OBS = 131072
NEX = 16
NEY = 64
N_GRP = 4
N_DEV = 8


def layout(key):
    peer_count = 2 * OBS_DEV // CAP
    group_count = TOTAL_OBS // (OBS_DEV * peer_count)
    cell_count = ELEM_DEV * SLOTS
    key_a, key_b, key_c, key_d, key_e = jax.random.split(key, 5)
    columns = jnp.arange(cell_count, dtype=jnp.int32)
    wanted = columns // CAP
    favored = jax.random.randint(key_a, (group_count, 1, 1), 0, peer_count, dtype=jnp.int32)
    jitter = jax.random.randint(key_b, (group_count, peer_count, cell_count), 1, 32768, dtype=jnp.int32)
    ranking = jnp.where(wanted[None, None, :] == favored, 0, jitter) * cell_count + columns
    picked = jnp.argsort(ranking, axis=-1)[:, :, :OBS_DEV].astype(jnp.int32)
    target = wanted[picked]
    row_ids = jnp.arange(OBS_DEV, dtype=jnp.int32)
    shuffle_keys = jax.random.randint(key_c, (group_count, peer_count, OBS_DEV), 0, 32768, dtype=jnp.int32) * OBS_DEV + row_ids
    mixing = jnp.argsort(shuffle_keys, axis=-1).astype(jnp.int32)
    target = jnp.take_along_axis(target, mixing, axis=-1)
    sorter = jnp.argsort(target, axis=-1, stable=True).astype(jnp.int32)
    sorted_target = jnp.take_along_axis(target, sorter, axis=-1)
    steps_row = jnp.broadcast_to(row_ids, sorted_target.shape)
    change = jnp.concatenate([jnp.ones((group_count, peer_count, 1), bool), sorted_target[:, :, 1:] != sorted_target[:, :, :-1]], axis=-1)
    starts = lax.cummax(jnp.where(change, steps_row, 0), axis=2)
    ranks_sorted = steps_row - starts
    inverse = jnp.argsort(sorter, axis=-1).astype(jnp.int32)
    send_slot = jnp.take_along_axis(ranks_sorted, inverse, axis=-1)
    owner = jnp.arange(group_count * peer_count, dtype=jnp.int32).reshape(group_count, peer_count, 1)
    segment = (owner * peer_count + target).reshape(-1)
    counts = jax.ops.segment_sum(jnp.ones_like(segment), segment, num_segments=group_count * peer_count * peer_count)
    counts = counts.reshape(group_count, peer_count, peer_count)
    earlier = jnp.cumsum(counts, axis=1) - counts
    arrival = jnp.take_along_axis(earlier, target, axis=2) + send_slot
    favored_elem = jax.random.randint(key_d, (group_count, peer_count, 1), 0, ELEM_DEV, dtype=jnp.int32)
    jitter_two = jax.random.randint(key_e, (group_count, peer_count, cell_count), 1, 32768, dtype=jnp.int32)
    ranking_two = jnp.where((columns // SLOTS)[None, None, :] == favored_elem, 0, jitter_two) * cell_count + columns
    table = jnp.argsort(ranking_two, axis=-1).astype(jnp.int32)
    group_ids = jnp.arange(group_count, dtype=jnp.int32).reshape(group_count, 1, 1)
    flat_index = ((group_ids * peer_count + target) * cell_count + arrival).reshape(-1)
    chosen = table.reshape(-1)[flat_index]
    return (target.reshape(-1).astype(jnp.int32), send_slot.reshape(-1).astype(jnp.int32), (chosen // SLOTS).astype(jnp.int32), (chosen % SLOTS).astype(jnp.int32))


def draw_obs_dest(key, part):
    return layout(jax.random.fold_in(key, 11))[0]


def draw_obs_send_slot(key, part):
    return layout(jax.random.fold_in(key, 11))[1]


def draw_obs_elem(key, part):
    return layout(jax.random.fold_in(key, 11))[2]


def draw_obs_slot(key, part):
    return layout(jax.random.fold_in(key, 11))[3]


def block_levels(stream_key, dims, pieces, smallest, top_value):
    level, own = 1.0, jax.random.fold_in(stream_key, 6)
    for dim, parts in pieces:
        draws = jnp.exp(jax.random.uniform(jax.random.fold_in(own, dim), (parts,), jnp.float32, smallest / len(pieces), top_value / len(pieces)))
        level = level * jnp.repeat(draws, dims[dim] // parts).reshape([-1 if axis == dim else 1 for axis in range(len(dims))])
    return level


def gaussian(stream_key, shape, width, reach, cuts=(), kind=jnp.bfloat16):
    loudness = block_levels(stream_key, shape, cuts, -0.22, 0.18) if cuts else 1.0
    array = jax.random.normal(stream_key, shape, jnp.float32) * width * loudness
    return jnp.minimum(jnp.maximum(array, -reach), reach).astype(kind)


def setup_inputs(seed: int = 0) -> dict:
    keys = jax.random.split(jax.random.key(seed), 8)
    obs_coord = jnp.clip(jax.random.uniform(keys[0], (3, TOTAL_OBS), jnp.float32, -1.0, 1.0) * block_levels(keys[0], (3, TOTAL_OBS), ((1, 32),), -0.4, 0.0), -1.0, 1.0)
    obs_resid = gaussian(keys[1], (TOTAL_OBS,), 1.0, 6.0, ((0, 32),), jnp.float32)
    obs_weight = jnp.clip(jnp.exp(math.log(2.0) - 1.3862944 * jax.random.uniform(keys[2], (TOTAL_OBS,), jnp.float32) ** block_levels(keys[2], (TOTAL_OBS,), ((0, 32),), -0.2, 0.2)), 0.5, 2.0)
    obs_dest = draw_obs_dest(jax.random.fold_in(keys[7], 71), 0)
    obs_send_slot = draw_obs_send_slot(jax.random.fold_in(keys[7], 71), 0)
    obs_elem = draw_obs_elem(jax.random.fold_in(keys[7], 71), 0)
    obs_slot = draw_obs_slot(jax.random.fold_in(keys[7], 71), 0)
    return {"obs_coord": obs_coord, "obs_resid": obs_resid, "obs_weight": obs_weight, "obs_dest": obs_dest, "obs_send_slot": obs_send_slot, "obs_elem": obs_elem, "obs_slot": obs_slot}


def basis_values(position):
    anchors = [-math.cos(math.pi * k / 7) for k in range(8)]
    basis = []
    for node_i in range(8):
        factor = jnp.ones_like(position)
        for node_m in range(8):
            if node_m != node_i:
                factor = factor * ((position - anchors[node_m]) / (anchors[node_i] - anchors[node_m]))
        basis.append(factor)
    return jnp.stack(basis)


def contract(first_w, second_w, third_w):
    outer = (first_w[:, None, :] * second_w[None, :, :]).reshape(64, ELEM_DEV, SLOTS)
    third = third_w.reshape(8, ELEM_DEV, SLOTS)
    mixed = jnp.einsum("aes,kes->eak", outer, third, precision=lax.Precision.HIGHEST)
    return mixed.reshape(ELEM_DEV, 512)


def combine(field, elem_dim, node_dim, from_low, from_high):
    count = field.shape[elem_dim]
    low_plane = lax.slice_in_dim(field, 0, 1, axis=node_dim)
    high_plane = lax.slice_in_dim(field, 7, 8, axis=node_dim)
    after = jnp.concatenate([lax.slice_in_dim(low_plane, 1, count, axis=elem_dim), from_high], axis=elem_dim)
    before = jnp.concatenate([from_low, lax.slice_in_dim(high_plane, 0, count - 1, axis=elem_dim)], axis=elem_dim)
    middle = lax.slice_in_dim(field, 1, 7, axis=node_dim)
    return jnp.concatenate([low_plane + before, middle, high_plane + after], axis=node_dim)


def block_nodes(block):
    first_w = basis_values(block[0]) * block[3]
    return contract(first_w, basis_values(block[1]), basis_values(block[2]))


def reference(obs_coord, obs_resid, obs_weight, obs_dest, obs_send_slot, obs_elem, obs_slot):
    forcing = obs_weight * obs_resid
    total_cost = 0.5 * jnp.sum(forcing * obs_resid)
    cell_count = ELEM_DEV * SLOTS
    device_count = N_GRP * N_DEV
    source = jnp.arange(TOTAL_OBS, dtype=jnp.int32) // OBS_DEV
    group_index = source // N_DEV
    device = group_index * N_DEV + obs_dest
    position = device * cell_count + obs_elem * SLOTS + obs_slot
    values = jnp.concatenate([obs_coord, forcing[None, :]], axis=0)
    packed = jnp.zeros((4, device_count * cell_count), obs_coord.dtype).at[:, position].set(values)
    blocks = packed.reshape(4, device_count, cell_count).transpose(1, 0, 2)
    raw = lax.map(block_nodes, blocks)
    raw = raw.reshape(N_GRP, N_DEV, EX, EY, EZ, 512).transpose(0, 2, 1, 3, 4, 5)
    field = raw.reshape(NEX, NEY, EZ, 8, 8, 8)
    for elem_dim in range(3):
        node_dim = elem_dim + 3
        edge = lax.slice_in_dim(lax.slice_in_dim(field, 0, 1, axis=node_dim), 0, 1, axis=elem_dim)
        empty = jnp.zeros_like(edge)
        field = combine(field, elem_dim, node_dim, empty, empty)
    return field.reshape(NEX, NEY, EZ, 512), total_cost
```

```python
import functools
import math

import jax
import jax.numpy as jnp
from jax import lax
from jax.experimental import pallas as pl
from jax.experimental.pallas import tpu as pltpu
from jax.sharding import PartitionSpec as P

EX = 4
EY = 8
EZ = 8
ELEM_DEV = 256
NODES = 8
FIELDS = 5
ANCHORS = [-math.cos(math.pi * k / 7) for k in range(NODES)]
SCALES = [
    1.0 / math.prod(ANCHORS[i] - ANCHORS[m] for m in range(NODES) if m != i) for i in range(NODES)
]
NT = (((1,), (1,)), ((), ()))


def pieces_of(values):
    first = values.astype(jnp.bfloat16)
    rest = values - first.astype(jnp.float32)
    second = rest.astype(jnp.bfloat16)
    third = rest - second.astype(jnp.float32)
    return [first.astype(jnp.float32), second.astype(jnp.float32), third]


def pack_kernel(coord, resid, weight, dest, slot, elem, out, acc, *, capacity, wide, chunk):
    rows = resid.shape[1]
    per_peer = capacity // wide
    high_count = 2 * rows // wide
    acc[...] = jnp.zeros_like(acc)
    lane_ids = lax.broadcasted_iota(jnp.int32, (wide, chunk), 0)

    def step(i, cost):
        at = pl.ds(pl.multiple_of(i * chunk, chunk), chunk)
        residual = resid[:, at]
        forcing = weight[:, at] * residual
        target = dest[:, at] * capacity + slot[:, at]
        high = target // wide
        low = target - high * wide
        right = jnp.where(lane_ids == low, 1.0, 0.0).astype(jnp.bfloat16)
        values = jnp.concatenate(
            [
                coord[:, at],
                forcing,
                elem[:, at].astype(jnp.float32),
                jnp.zeros((8 - FIELDS, chunk), jnp.float32),
            ],
            axis=0,
        )
        high_rep = jnp.broadcast_to(high, (8, chunk))
        pieces = pieces_of(values)
        total = None
        for piece in pieces:
            left = jnp.concatenate(
                [jnp.where(high_rep == h, piece, 0.0) for h in range(high_count)], axis=0
            ).astype(jnp.bfloat16)
            part = lax.dot_general(left, right, NT, preferred_element_type=jnp.float32)
            total = part if total is None else total + part
        acc[...] += total
        return cost + forcing * residual

    cost = lax.fori_loop(0, rows // chunk, step, jnp.zeros((1, chunk), jnp.float32))
    cost = 0.5 * jnp.sum(cost, axis=1, keepdims=True)
    used = FIELDS * per_peer
    for peer in range(out.shape[0]):
        for j in range(per_peer):
            source = (peer * per_peer + j) * 8
            out[peer, FIELDS * j : FIELDS * (j + 1), :] = acc[source : source + FIELDS, :]
        out[peer, used:, :] = jnp.broadcast_to(cost, (out.shape[1] - used, wide))


def basis_of(position, node, scale):
    factor = scale
    for m in range(NODES):
        factor = factor * jnp.where(node == m, 1.0, position - ANCHORS[m])
    return factor


def field_kernel(got, field, planes, acc, elems, first, second, *, capacity, wide, block):
    peer_count = got.shape[0]
    per_peer = capacity // wide
    parts = block // wide
    node = lax.broadcasted_iota(jnp.int32, (NODES, wide), 0)
    scale = jnp.zeros((NODES, wide), jnp.float32)
    for i in range(NODES):
        scale = jnp.where(node == i, SCALES[i], scale)
    elem_ids = lax.broadcasted_iota(jnp.int32, (ELEM_DEV, wide), 0).astype(jnp.float32)
    acc[...] = jnp.zeros_like(acc)

    def step(i, carry):
        for q in range(parts):
            peer = i * (parts // per_peer) + q // per_peer
            row = FIELDS * (q % per_peer)
            u, v, w, f, e = (got[peer, row + k : row + k + 1, :] for k in range(FIELDS))
            lanes = slice(q * wide, (q + 1) * wide)
            elems[:, lanes] = jnp.where(elem_ids == e, 1.0, 0.0).astype(jnp.bfloat16)
            first_w = basis_of(u, node, scale) * f
            second_w = basis_of(v, node, scale)
            third_w = basis_of(w, node, scale)
            inner = [second_w[b : b + 1, :] * third_w for b in range(NODES)]
            for a in range(NODES):
                mine = jnp.broadcast_to(first_w[a : a + 1, :], (NODES, wide))
                whole = jnp.concatenate([mine * inner[b] for b in range(NODES)], axis=0)
                head = whole.astype(jnp.bfloat16)
                at = slice(64 * a, 64 * (a + 1))
                first[at, lanes] = head
                second[at, lanes] = (whole - head.astype(jnp.float32)).astype(jnp.bfloat16)
        chosen = elems[...]
        acc[...] += lax.dot_general(
            chosen, first[...], NT, preferred_element_type=jnp.float32
        ) + lax.dot_general(chosen, second[...], NT, preferred_element_type=jnp.float32)
        return carry

    lax.fori_loop(0, peer_count * capacity // block, step, 0)

    lane = lax.broadcasted_iota(jnp.int32, (EZ, 128), 1)
    level = lax.broadcasted_iota(jnp.int32, (EZ, 128), 0)
    take_up = jnp.logical_and(lane % 8 == 7, level < EZ - 1)
    take_down = jnp.logical_and(lane % 8 == 0, level > 0)
    columns = []
    for j in range(4):
        blocks = []
        for r in range(EX * EY):
            x = acc[8 * r : 8 * (r + 1), 128 * j : 128 * (j + 1)]
            up = pltpu.roll(pltpu.roll(x, EZ - 1, 0), 7, 1)
            down = pltpu.roll(pltpu.roll(x, 1, 0), 121, 1)
            blocks.append(x + jnp.where(take_up, up, 0.0) + jnp.where(take_down, down, 0.0))
        column = []
        for r in range(EX * EY):
            x = blocks[r]
            if r % EY < EY - 1:
                x = x + jnp.where(lane % 64 >= 56, pltpu.roll(blocks[r + 1], 56, 1), 0.0)
            if r % EY > 0:
                x = x + jnp.where(lane % 64 < 8, pltpu.roll(blocks[r - 1], 72, 1), 0.0)
            column.append(x)
        if j in (1, 2):
            for r in range(EX * EY):
                field[8 * r : 8 * (r + 1), 128 * j : 128 * (j + 1)] = column[r]
        columns.append(column)
    lower, upper = columns[0], columns[3]
    for r in range(EX * EY):
        x, y = lower[r], upper[r]
        if r >= EY:
            x = x + jnp.where(lane < 64, pltpu.roll(upper[r - EY], 64, 1), 0.0)
        if r < (EX - 1) * EY:
            y = y + jnp.where(lane >= 64, pltpu.roll(lower[r + EY], 64, 1), 0.0)
        field[8 * r : 8 * (r + 1), 0:128] = x
        field[8 * r : 8 * (r + 1), 384:512] = y
    half = EY // 2
    mine = lax.axis_index("grp")
    used = FIELDS * per_peer
    cost = got[0, used : used + 1, 0:128]
    for peer in range(1, peer_count):
        cost = cost + got[peer, used : used + 1, 0:128]
    last = (EX - 1) * EY
    for r in range(half):
        low_pack = jnp.where(lane < 64, lower[r], pltpu.roll(lower[r + half], 64, 1))
        high_pack = jnp.where(
            lane < 64, pltpu.roll(upper[last + r], 64, 1), upper[last + r + half]
        )
        for other in range(planes.shape[0]):
            message = jnp.where(other == mine - 1, low_pack, 0.0)
            planes[other, 8 * r : 8 * (r + 1), :] = jnp.where(other == mine + 1, high_pack, message)
    for other in range(planes.shape[0]):
        planes[other, 8 * half :, :] = jnp.broadcast_to(cost, (8, 128))


def neighbours(planes, lane, r):
    count = planes.shape[0]
    half = EY // 2
    mine = lax.axis_index("grp")
    below = jnp.maximum(mine - 1, 0)
    above = jnp.minimum(mine + 1, count - 1)
    at = 8 * (r % half)
    low = planes[below, at : at + 8, :]
    high = planes[above, at : at + 8, :]
    if r >= half:
        low = pltpu.roll(low, 64, 1)
    else:
        high = pltpu.roll(high, 64, 1)
    low = jnp.where(jnp.logical_and(lane < 64, mine > 0), low, 0.0)
    high = jnp.where(jnp.logical_and(lane >= 64, mine < count - 1), high, 0.0)
    return low, high


def edge_kernel(field, planes, to_low, to_high, cost):
    lane = lax.broadcasted_iota(jnp.int32, (EZ, 128), 1)
    for ex in range(EX):
        for r, out, shift in ((0, to_low, 0), (EY - 1, to_high, 72)):
            rows = 8 * (ex * EY + r)
            mask = lane % 64 >= 56 if shift else lane % 64 < 8
            total = jnp.zeros((EZ, 128), jnp.float32)
            for j in range(4):
                x = field[rows : rows + 8, 128 * j : 128 * (j + 1)]
                if ex == 0 and j == 0:
                    x = x + neighbours(planes, lane, r)[0]
                if ex == EX - 1 and j == 3:
                    x = x + neighbours(planes, lane, r)[1]
                x = jnp.where(mask, x, 0.0)
                move = (shift + 8 * j) % 128
                total = total + (pltpu.roll(x, move, 1) if move else x)
            out[8 * ex : 8 * (ex + 1), :] = total
    total = planes[0, 4 * EY : 4 * EY + 1, :]
    for other in range(1, planes.shape[0]):
        total = total + planes[other, 4 * EY : 4 * EY + 1, :]
    cost[...] = total


def finish_kernel(field, planes, from_low, from_high, out):
    lane = lax.broadcasted_iota(jnp.int32, (EZ, 128), 1)
    for ex in range(EX):
        for r in range(EY):
            rows = 8 * (ex * EY + r)
            for j in range(4):
                x = field[rows : rows + 8, 128 * j : 128 * (j + 1)]
                if ex == 0 and j == 0:
                    x = x + neighbours(planes, lane, r)[0]
                if ex == EX - 1 and j == 3:
                    x = x + neighbours(planes, lane, r)[1]
                if r == 0:
                    part = from_low[8 * ex : 8 * (ex + 1), :]
                    move = (128 - 8 * j) % 128
                    part = pltpu.roll(part, move, 1) if move else part
                    x = x + jnp.where(lane % 64 < 8, part, 0.0)
                if r == EY - 1:
                    part = from_high[8 * ex : 8 * (ex + 1), :]
                    x = x + jnp.where(lane % 64 >= 56, pltpu.roll(part, 56 - 8 * j, 1), 0.0)
                out[rows : rows + 8, 128 * j : 128 * (j + 1)] = x


def on_device(obs_coord, obs_resid, obs_weight, obs_dest, obs_send_slot, obs_elem, obs_slot):
    peer_count = lax.axis_size("dev")
    group_count = lax.axis_size("grp")
    row_count = obs_resid.shape[0]
    capacity = 2 * row_count // peer_count
    wide = min(256, capacity)
    per_peer = capacity // wide
    message_rows = -(-(FIELDS * per_peer + 1) // 8) * 8
    block = 1024
    f32 = jnp.float32
    flat = [a.reshape(1, row_count) for a in (obs_resid, obs_weight, obs_dest, obs_send_slot, obs_elem)]
    send = pl.pallas_call(
        functools.partial(pack_kernel, capacity=capacity, wide=wide, chunk=512),
        out_shape=jax.ShapeDtypeStruct((peer_count, message_rows, wide), f32),
        scratch_shapes=[pltpu.VMEM((2 * row_count // wide * 8, wide), f32)],
        name="pack",
    )(obs_coord, *flat)
    got = lax.all_to_all(send, "dev", split_axis=0, concat_axis=0, tiled=True)
    field, planes = pl.pallas_call(
        functools.partial(field_kernel, capacity=capacity, wide=wide, block=block),
        out_shape=(
            jax.ShapeDtypeStruct((ELEM_DEV, 512), f32),
            jax.ShapeDtypeStruct((group_count, 4 * EY + 8, 128), f32),
        ),
        scratch_shapes=[
            pltpu.VMEM((ELEM_DEV, 512), f32),
            pltpu.VMEM((ELEM_DEV, block), jnp.bfloat16),
            pltpu.VMEM((512, block), jnp.bfloat16),
            pltpu.VMEM((512, block), jnp.bfloat16),
        ],
        name="field",
    )(got)
    planes = lax.all_to_all(planes, "grp", split_axis=0, concat_axis=0, tiled=True)
    edge = jax.ShapeDtypeStruct((EX * EZ, 128), f32)
    to_low, to_high, cost = pl.pallas_call(
        edge_kernel,
        out_shape=(edge, edge, jax.ShapeDtypeStruct((1, 128), f32)),
        name="edge",
    )(field, planes)
    forward = [(i, i + 1) for i in range(peer_count - 1)]
    backward = [(target, source) for source, target in forward]
    from_low = lax.ppermute(to_high, "dev", forward)
    from_high = lax.ppermute(to_low, "dev", backward)
    nodal = pl.pallas_call(
        finish_kernel,
        out_shape=jax.ShapeDtypeStruct((ELEM_DEV, 512), f32),
        name="finish",
    )(field, planes, from_low, from_high)
    return (nodal.reshape(EX, EY, EZ, 512), cost[0, 0])


def solution(mesh):
    placed = (
        P(None, ("grp", "dev")),
        P(("grp", "dev")),
        P(("grp", "dev")),
        P(("grp", "dev")),
        P(("grp", "dev")),
        P(("grp", "dev")),
        P(("grp", "dev")),
    )
    return jax.shard_map(
        on_device,
        mesh=mesh,
        in_specs=placed,
        out_specs=(P("grp", "dev", None, None), P()),
        check_vma=False,
    )
```

```python
import functools
import math

import jax
import jax.numpy as jnp
from jax import lax
from jax.experimental import pallas as pl
from jax.experimental.pallas import tpu as pltpu
from jax.sharding import PartitionSpec as P

EX = 4
EY = 8
EZ = 8
ELEM_DEV = 256
NODES = 8
FIELDS = 5
PIECES = 3
ANCHORS = [-math.cos(math.pi * k / 7) for k in range(NODES)]
SCALES = [
    1.0 / math.prod(ANCHORS[i] - ANCHORS[m] for m in range(NODES) if m != i) for i in range(NODES)
]
NT = (((1,), (1,)), ((), ()))


def pieces_of(values):
    first = values.astype(jnp.bfloat16)
    rest = values - first.astype(jnp.float32)
    second = rest.astype(jnp.bfloat16)
    third = rest - second.astype(jnp.float32)
    return [first.astype(jnp.float32), second.astype(jnp.float32), third]


def pack_kernel(coord, resid, weight, dest, slot, elem, out, acc, *, capacity, wide, chunk):
    rows = resid.shape[1]
    per_peer = capacity // wide
    high_count = 2 * rows // wide
    acc[...] = jnp.zeros_like(acc)
    lane_ids = lax.broadcasted_iota(jnp.int32, (wide, chunk), 0)
    high_ids = lax.broadcasted_iota(jnp.int32, (high_count, chunk), 0)

    def step(i, cost):
        at = pl.ds(pl.multiple_of(i * chunk, chunk), chunk)
        residual = resid[:, at]
        forcing = weight[:, at] * residual
        target = dest[:, at] * capacity + slot[:, at]
        high = target // wide
        low = target - high * wide
        right = jnp.where(lane_ids == low, 1.0, 0.0).astype(jnp.bfloat16)
        chosen = high_ids == high
        pieces = pieces_of(jnp.concatenate([coord[:, at], forcing], axis=0))
        lines = [piece[k : k + 1, :] for k in range(FIELDS - 1) for piece in pieces]
        lines.append(elem[:, at].astype(jnp.float32))
        left = jnp.concatenate(
            [
                jnp.where(chosen, jnp.broadcast_to(line, chosen.shape), 0.0).astype(jnp.bfloat16)
                for line in lines
            ],
            axis=0,
        )
        acc[...] += lax.dot_general(left, right, NT, preferred_element_type=jnp.float32)
        return cost + forcing * residual

    cost = lax.fori_loop(0, rows // chunk, step, jnp.zeros((1, chunk), jnp.float32))
    cost = 0.5 * jnp.sum(cost, axis=1, keepdims=True)
    used = FIELDS * per_peer
    for k in range(FIELDS):
        base = k * PIECES * high_count
        total = acc[base : base + high_count, :]
        for p in range(1, PIECES if k < FIELDS - 1 else 1):
            total = total + acc[base + p * high_count : base + (p + 1) * high_count, :]
        for peer in range(out.shape[0]):
            out[peer, k * per_peer : (k + 1) * per_peer, :] = total[
                peer * per_peer : (peer + 1) * per_peer, :
            ]
    for peer in range(out.shape[0]):
        out[peer, used:, :] = jnp.broadcast_to(cost, (out.shape[1] - used, wide))


def basis_of(position, node, scale):
    factor = scale
    for m in range(NODES):
        factor = factor * jnp.where(node == m, 1.0, position - ANCHORS[m])
    return factor


def field_kernel(got, field, planes, acc, raw, elems, outer, *, capacity, wide, block):
    peer_count = got.shape[0]
    per_peer = capacity // wide
    parts = block // wide
    node = lax.broadcasted_iota(jnp.int32, (NODES, wide), 0)
    scale = jnp.zeros((NODES, wide), jnp.float32)
    for i in range(NODES):
        scale = jnp.where(node == i, SCALES[i], scale)
    elem_ids = lax.broadcasted_iota(jnp.int32, (ELEM_DEV, wide), 0).astype(jnp.float32)
    acc[...] = jnp.zeros_like(acc)

    def step(i, carry):
        for q in range(parts):
            peer = i * (parts // per_peer) + q // per_peer
            row = q % per_peer
            u, v, w, f, e = (
                got[peer, row + k * per_peer : row + k * per_peer + 1, :] for k in range(FIELDS)
            )
            lanes = slice(q * wide, (q + 1) * wide)
            elems[:, lanes] = jnp.where(elem_ids == e, 1.0, 0.0).astype(jnp.bfloat16)
            first_w = basis_of(u, node, scale) * f
            second_w = basis_of(v, node, scale)
            third_w = basis_of(w, node, scale)
            inner = [second_w[b : b + 1, :] * third_w for b in range(NODES)]
            for a in range(NODES):
                mine = jnp.broadcast_to(first_w[a : a + 1, :], (NODES, wide))
                whole = jnp.concatenate([mine * inner[b] for b in range(NODES)], axis=0)
                head = whole.astype(jnp.bfloat16)
                rest = (whole - head.astype(jnp.float32)).astype(jnp.bfloat16)
                outer[64 * a : 64 * (a + 1), lanes] = head
                outer[512 + 64 * a : 512 + 64 * (a + 1), lanes] = rest
        acc[...] += lax.dot_general(
            outer[...], elems[...], NT, preferred_element_type=jnp.float32
        )
        return carry

    lax.fori_loop(0, peer_count * capacity // block, step, 0)
    raw[...] = (acc[:512] + acc[512:]).T

    lane = lax.broadcasted_iota(jnp.int32, (EZ, 128), 1)
    level = lax.broadcasted_iota(jnp.int32, (EZ, 128), 0)
    take_up = jnp.logical_and(lane % 8 == 7, level < EZ - 1)
    take_down = jnp.logical_and(lane % 8 == 0, level > 0)
    columns = []
    for j in range(4):
        blocks = []
        for r in range(EX * EY):
            x = raw[8 * r : 8 * (r + 1), 128 * j : 128 * (j + 1)]
            up = pltpu.roll(pltpu.roll(x, EZ - 1, 0), 7, 1)
            down = pltpu.roll(pltpu.roll(x, 1, 0), 121, 1)
            blocks.append(x + jnp.where(take_up, up, 0.0) + jnp.where(take_down, down, 0.0))
        column = []
        for r in range(EX * EY):
            x = blocks[r]
            if r % EY < EY - 1:
                x = x + jnp.where(lane % 64 >= 56, pltpu.roll(blocks[r + 1], 56, 1), 0.0)
            if r % EY > 0:
                x = x + jnp.where(lane % 64 < 8, pltpu.roll(blocks[r - 1], 72, 1), 0.0)
            column.append(x)
        if j in (1, 2):
            for r in range(EX * EY):
                field[8 * r : 8 * (r + 1), 128 * j : 128 * (j + 1)] = column[r]
        columns.append(column)
    lower, upper = columns[0], columns[3]
    for r in range(EX * EY):
        x, y = lower[r], upper[r]
        if r >= EY:
            x = x + jnp.where(lane < 64, pltpu.roll(upper[r - EY], 64, 1), 0.0)
        if r < (EX - 1) * EY:
            y = y + jnp.where(lane >= 64, pltpu.roll(lower[r + EY], 64, 1), 0.0)
        field[8 * r : 8 * (r + 1), 0:128] = x
        field[8 * r : 8 * (r + 1), 384:512] = y
    half = EY // 2
    mine = lax.axis_index("grp")
    used = FIELDS * per_peer
    cost = got[0, used : used + 1, 0:128]
    for peer in range(1, peer_count):
        cost = cost + got[peer, used : used + 1, 0:128]
    last = (EX - 1) * EY
    for r in range(half):
        low_pack = jnp.where(lane < 64, lower[r], pltpu.roll(lower[r + half], 64, 1))
        high_pack = jnp.where(
            lane < 64, pltpu.roll(upper[last + r], 64, 1), upper[last + r + half]
        )
        for other in range(planes.shape[0]):
            message = jnp.where(other == mine - 1, low_pack, 0.0)
            planes[other, 8 * r : 8 * (r + 1), :] = jnp.where(other == mine + 1, high_pack, message)
    for other in range(planes.shape[0]):
        planes[other, 8 * half :, :] = jnp.broadcast_to(cost, (8, 128))


def neighbours(planes, lane, r):
    count = planes.shape[0]
    half = EY // 2
    mine = lax.axis_index("grp")
    below = jnp.maximum(mine - 1, 0)
    above = jnp.minimum(mine + 1, count - 1)
    at = 8 * (r % half)
    low = planes[below, at : at + 8, :]
    high = planes[above, at : at + 8, :]
    if r >= half:
        low = pltpu.roll(low, 64, 1)
    else:
        high = pltpu.roll(high, 64, 1)
    low = jnp.where(jnp.logical_and(lane < 64, mine > 0), low, 0.0)
    high = jnp.where(jnp.logical_and(lane >= 64, mine < count - 1), high, 0.0)
    return low, high


def edge_kernel(field, planes, to_low, to_high, cost):
    lane = lax.broadcasted_iota(jnp.int32, (EZ, 128), 1)
    for ex in range(EX):
        for r, out, shift in ((0, to_low, 0), (EY - 1, to_high, 72)):
            rows = 8 * (ex * EY + r)
            mask = lane % 64 >= 56 if shift else lane % 64 < 8
            total = jnp.zeros((EZ, 128), jnp.float32)
            for j in range(4):
                x = field[rows : rows + 8, 128 * j : 128 * (j + 1)]
                if ex == 0 and j == 0:
                    x = x + neighbours(planes, lane, r)[0]
                if ex == EX - 1 and j == 3:
                    x = x + neighbours(planes, lane, r)[1]
                x = jnp.where(mask, x, 0.0)
                move = (shift + 8 * j) % 128
                total = total + (pltpu.roll(x, move, 1) if move else x)
            out[8 * ex : 8 * (ex + 1), :] = total
    total = planes[0, 4 * EY : 4 * EY + 1, :]
    for other in range(1, planes.shape[0]):
        total = total + planes[other, 4 * EY : 4 * EY + 1, :]
    cost[...] = total


def finish_kernel(field, planes, from_low, from_high, out):
    lane = lax.broadcasted_iota(jnp.int32, (EZ, 128), 1)
    for ex in range(EX):
        for r in range(EY):
            rows = 8 * (ex * EY + r)
            for j in range(4):
                x = field[rows : rows + 8, 128 * j : 128 * (j + 1)]
                if ex == 0 and j == 0:
                    x = x + neighbours(planes, lane, r)[0]
                if ex == EX - 1 and j == 3:
                    x = x + neighbours(planes, lane, r)[1]
                if r == 0:
                    part = from_low[8 * ex : 8 * (ex + 1), :]
                    move = (128 - 8 * j) % 128
                    part = pltpu.roll(part, move, 1) if move else part
                    x = x + jnp.where(lane % 64 < 8, part, 0.0)
                if r == EY - 1:
                    part = from_high[8 * ex : 8 * (ex + 1), :]
                    x = x + jnp.where(lane % 64 >= 56, pltpu.roll(part, 56 - 8 * j, 1), 0.0)
                out[rows : rows + 8, 128 * j : 128 * (j + 1)] = x


def in_vmem(array):
    return pltpu.with_memory_space_constraint(array, pltpu.VMEM)


def on_device(obs_coord, obs_resid, obs_weight, obs_dest, obs_send_slot, obs_elem, obs_slot):
    peer_count = lax.axis_size("dev")
    group_count = lax.axis_size("grp")
    row_count = obs_resid.shape[0]
    capacity = 2 * row_count // peer_count
    wide = min(256, capacity)
    per_peer = capacity // wide
    message_rows = -(-(FIELDS * per_peer + 1) // 8) * 8
    block = 2 * row_count
    lines = (FIELDS - 1) * PIECES + 1
    f32 = jnp.float32
    flat = [a.reshape(1, row_count) for a in (obs_resid, obs_weight, obs_dest, obs_send_slot, obs_elem)]
    send = pl.pallas_call(
        functools.partial(pack_kernel, capacity=capacity, wide=wide, chunk=row_count),
        out_shape=pltpu.VMEM((peer_count, message_rows, wide), f32),
        scratch_shapes=[pltpu.VMEM((lines * 2 * row_count // wide, wide), f32)],
        name="pack",
    )(obs_coord, *flat)
    got = lax.all_to_all(send, "dev", split_axis=0, concat_axis=0, tiled=True)
    field, planes = pl.pallas_call(
        functools.partial(field_kernel, capacity=capacity, wide=wide, block=block),
        out_shape=(
            pltpu.VMEM((ELEM_DEV, 512), f32),
            pltpu.VMEM((group_count, 4 * EY + 8, 128), f32),
        ),
        scratch_shapes=[
            pltpu.VMEM((2 * 512, ELEM_DEV), f32),
            pltpu.VMEM((ELEM_DEV, 512), f32),
            pltpu.VMEM((ELEM_DEV, block), jnp.bfloat16),
            pltpu.VMEM((2 * 512, block), jnp.bfloat16),
        ],
        name="field",
    )(in_vmem(got))
    planes = lax.all_to_all(planes, "grp", split_axis=0, concat_axis=0, tiled=True)
    edge = pltpu.VMEM((EX * EZ, 128), f32)
    field, planes = in_vmem(field), in_vmem(planes)
    to_low, to_high, cost = pl.pallas_call(
        edge_kernel,
        out_shape=(edge, edge, jax.ShapeDtypeStruct((1, 128), f32)),
        name="edge",
    )(field, planes)
    forward = [(i, i + 1) for i in range(peer_count - 1)]
    backward = [(target, source) for source, target in forward]
    from_low = lax.ppermute(to_high, "dev", forward)
    from_high = lax.ppermute(to_low, "dev", backward)
    nodal = pl.pallas_call(
        finish_kernel,
        out_shape=jax.ShapeDtypeStruct((ELEM_DEV, 512), f32),
        name="finish",
    )(field, planes, in_vmem(from_low), in_vmem(from_high))
    return (nodal.reshape(EX, EY, EZ, 512), cost[0, 0])


def solution(mesh):
    placed = (
        P(None, ("grp", "dev")),
        P(("grp", "dev")),
        P(("grp", "dev")),
        P(("grp", "dev")),
        P(("grp", "dev")),
        P(("grp", "dev")),
        P(("grp", "dev")),
    )
    return jax.shard_map(
        on_device,
        mesh=mesh,
        in_specs=placed,
        out_specs=(P("grp", "dev", None, None), P()),
        check_vma=False,
    )
```

```python
import functools
import math

import jax
import jax.numpy as jnp
from jax import lax
from jax.experimental import pallas as pl
from jax.experimental.pallas import tpu as pltpu
from jax.sharding import PartitionSpec as P

EX = 4
EY = 8
EZ = 8
ELEM_DEV = 256
NODES = 8
FIELDS = 5
PIECES = 3
ANCHORS = [-math.cos(math.pi * k / 7) for k in range(NODES)]
SCALES = [
    1.0 / math.prod(ANCHORS[i] - ANCHORS[m] for m in range(NODES) if m != i) for i in range(NODES)
]
NT = (((1,), (1,)), ((), ()))


def pieces_of(values):
    first = values.astype(jnp.bfloat16)
    rest = values - first.astype(jnp.float32)
    second = rest.astype(jnp.bfloat16)
    third = rest - second.astype(jnp.float32)
    return [first.astype(jnp.float32), second.astype(jnp.float32), third]


def pack_kernel(coord, resid, weight, dest, slot, elem, out, acc, *, capacity, wide, chunk):
    rows = resid.shape[1]
    per_peer = capacity // wide
    high_count = 2 * rows // wide
    acc[...] = jnp.zeros_like(acc)
    lane_ids = lax.broadcasted_iota(jnp.int32, (wide, chunk), 0)
    high_ids = lax.broadcasted_iota(jnp.int32, (high_count, chunk), 0)

    def step(i, cost):
        at = pl.ds(pl.multiple_of(i * chunk, chunk), chunk)
        residual = resid[:, at]
        forcing = weight[:, at] * residual
        target = dest[:, at] * capacity + slot[:, at]
        high = target // wide
        low = target - high * wide
        right = jnp.where(lane_ids == low, 1.0, 0.0).astype(jnp.bfloat16)
        chosen = high_ids == high
        pieces = pieces_of(jnp.concatenate([coord[:, at], forcing], axis=0))
        lines = [piece[k : k + 1, :] for k in range(FIELDS - 1) for piece in pieces]
        lines.append(elem[:, at].astype(jnp.float32))
        left = jnp.concatenate(
            [
                jnp.where(chosen, jnp.broadcast_to(line, chosen.shape), 0.0).astype(jnp.bfloat16)
                for line in lines
            ],
            axis=0,
        )
        acc[...] += lax.dot_general(left, right, NT, preferred_element_type=jnp.float32)
        return cost + forcing * residual

    cost = lax.fori_loop(0, rows // chunk, step, jnp.zeros((1, chunk), jnp.float32))
    cost = 0.5 * jnp.sum(cost, axis=1, keepdims=True)
    used = FIELDS * per_peer
    for k in range(FIELDS):
        base = k * PIECES * high_count
        total = acc[base : base + high_count, :]
        for p in range(1, PIECES if k < FIELDS - 1 else 1):
            total = total + acc[base + p * high_count : base + (p + 1) * high_count, :]
        for peer in range(out.shape[0]):
            out[peer, k * per_peer : (k + 1) * per_peer, :] = total[
                peer * per_peer : (peer + 1) * per_peer, :
            ]
    for peer in range(out.shape[0]):
        out[peer, used:, :] = jnp.broadcast_to(cost, (out.shape[1] - used, wide))


def basis_of(position, node, scale):
    factor = scale
    for m in range(NODES):
        factor = factor * jnp.where(node == m, 1.0, position - ANCHORS[m])
    return factor


def field_kernel(got, field, to_below, to_above, cost, acc, raw, elems, outer, *, capacity, wide, block):
    peer_count = got.shape[0]
    per_peer = capacity // wide
    parts = block // wide
    node = lax.broadcasted_iota(jnp.int32, (NODES, wide), 0)
    scale = jnp.zeros((NODES, wide), jnp.float32)
    for i in range(NODES):
        scale = jnp.where(node == i, SCALES[i], scale)
    elem_ids = lax.broadcasted_iota(jnp.int32, (ELEM_DEV, wide), 0).astype(jnp.float32)
    acc[...] = jnp.zeros_like(acc)

    def step(i, carry):
        for q in range(parts):
            peer = i * (parts // per_peer) + q // per_peer
            row = q % per_peer
            u, v, w, f, e = (
                got[peer, row + k * per_peer : row + k * per_peer + 1, :] for k in range(FIELDS)
            )
            lanes = slice(q * wide, (q + 1) * wide)
            elems[:, lanes] = jnp.where(elem_ids == e, 1.0, 0.0).astype(jnp.bfloat16)
            first_w = basis_of(u, node, scale) * f
            second_w = basis_of(v, node, scale)
            third_w = basis_of(w, node, scale)
            inner = [second_w[b : b + 1, :] * third_w for b in range(NODES)]
            for a in range(NODES):
                mine = jnp.broadcast_to(first_w[a : a + 1, :], (NODES, wide))
                whole = jnp.concatenate([mine * inner[b] for b in range(NODES)], axis=0)
                head = whole.astype(jnp.bfloat16)
                rest = (whole - head.astype(jnp.float32)).astype(jnp.bfloat16)
                outer[64 * a : 64 * (a + 1), lanes] = head
                outer[512 + 64 * a : 512 + 64 * (a + 1), lanes] = rest
        acc[...] += lax.dot_general(
            outer[...], elems[...], NT, preferred_element_type=jnp.float32
        )
        return carry

    lax.fori_loop(0, peer_count * capacity // block, step, 0)
    raw[...] = (acc[:512] + acc[512:]).T

    lane = lax.broadcasted_iota(jnp.int32, (EZ, 128), 1)
    level = lax.broadcasted_iota(jnp.int32, (EZ, 128), 0)
    take_up = jnp.logical_and(lane % 8 == 7, level < EZ - 1)
    take_down = jnp.logical_and(lane % 8 == 0, level > 0)
    columns = []
    for j in range(4):
        blocks = []
        for r in range(EX * EY):
            x = raw[8 * r : 8 * (r + 1), 128 * j : 128 * (j + 1)]
            up = pltpu.roll(pltpu.roll(x, EZ - 1, 0), 7, 1)
            down = pltpu.roll(pltpu.roll(x, 1, 0), 121, 1)
            blocks.append(x + jnp.where(take_up, up, 0.0) + jnp.where(take_down, down, 0.0))
        column = []
        for r in range(EX * EY):
            x = blocks[r]
            if r % EY < EY - 1:
                x = x + jnp.where(lane % 64 >= 56, pltpu.roll(blocks[r + 1], 56, 1), 0.0)
            if r % EY > 0:
                x = x + jnp.where(lane % 64 < 8, pltpu.roll(blocks[r - 1], 72, 1), 0.0)
            column.append(x)
        if j in (1, 2):
            for r in range(EX * EY):
                field[8 * r : 8 * (r + 1), 128 * j : 128 * (j + 1)] = column[r]
        columns.append(column)
    lower, upper = columns[0], columns[3]
    for r in range(EX * EY):
        x, y = lower[r], upper[r]
        if r >= EY:
            x = x + jnp.where(lane < 64, pltpu.roll(upper[r - EY], 64, 1), 0.0)
        if r < (EX - 1) * EY:
            y = y + jnp.where(lane >= 64, pltpu.roll(lower[r + EY], 64, 1), 0.0)
        field[8 * r : 8 * (r + 1), 0:128] = x
        field[8 * r : 8 * (r + 1), 384:512] = y
    half = EY // 2
    used = FIELDS * per_peer
    total = got[0, used : used + 1, 0:128]
    for peer in range(1, peer_count):
        total = total + got[peer, used : used + 1, 0:128]
    total = jnp.broadcast_to(total, (8, 128))
    last = (EX - 1) * EY
    for r in range(half):
        to_below[8 * r : 8 * (r + 1), :] = jnp.where(
            lane < 64, lower[r], pltpu.roll(lower[r + half], 64, 1)
        )
        to_above[8 * r : 8 * (r + 1), :] = jnp.where(
            lane < 64, pltpu.roll(upper[last + r], 64, 1), upper[last + r + half]
        )
    to_below[8 * half :, :] = total
    to_above[8 * half :, :] = total
    cost[...] = total


def neighbours(from_below, from_above, lane, r):
    count = lax.axis_size("grp")
    half = EY // 2
    mine = lax.axis_index("grp")
    at = 8 * (r % half)
    low = from_below[at : at + 8, :]
    high = from_above[at : at + 8, :]
    if r >= half:
        low = pltpu.roll(low, 64, 1)
    else:
        high = pltpu.roll(high, 64, 1)
    low = jnp.where(jnp.logical_and(lane < 64, mine > 0), low, 0.0)
    high = jnp.where(jnp.logical_and(lane >= 64, mine < count - 1), high, 0.0)
    return low, high


def edge_kernel(field, from_below, from_above, *rest):
    *costs, to_low, to_high, cost = rest
    lane = lax.broadcasted_iota(jnp.int32, (EZ, 128), 1)
    for ex in range(EX):
        for r, out, shift in ((0, to_low, 0), (EY - 1, to_high, 72)):
            rows = 8 * (ex * EY + r)
            mask = lane % 64 >= 56 if shift else lane % 64 < 8
            total = jnp.zeros((EZ, 128), jnp.float32)
            for j in range(4):
                x = field[rows : rows + 8, 128 * j : 128 * (j + 1)]
                if ex == 0 and j == 0:
                    x = x + neighbours(from_below, from_above, lane, r)[0]
                if ex == EX - 1 and j == 3:
                    x = x + neighbours(from_below, from_above, lane, r)[1]
                x = jnp.where(mask, x, 0.0)
                move = (shift + 8 * j) % 128
                total = total + (pltpu.roll(x, move, 1) if move else x)
            out[8 * ex : 8 * (ex + 1), :] = total
    count = lax.axis_size("grp")
    mine = lax.axis_index("grp")
    row = slice(4 * EY, 4 * EY + 1)
    known = [costs[0][0:1, :], from_below[row, :], from_above[row, :]]
    known += [other[0:1, :] for other in costs[1:]]
    shifts = [0, count - 1, 1] + list(range(2, count - 1))
    total = jnp.zeros((1, 128), jnp.float32)
    for group in range(count):
        for shift, value in zip(shifts, known):
            total = total + jnp.where((mine + shift) % count == group, value, 0.0)
    cost[...] = total


def finish_kernel(field, from_below, from_above, from_low, from_high, out):
    lane = lax.broadcasted_iota(jnp.int32, (EZ, 128), 1)
    for ex in range(EX):
        for r in range(EY):
            rows = 8 * (ex * EY + r)
            for j in range(4):
                x = field[rows : rows + 8, 128 * j : 128 * (j + 1)]
                if ex == 0 and j == 0:
                    x = x + neighbours(from_below, from_above, lane, r)[0]
                if ex == EX - 1 and j == 3:
                    x = x + neighbours(from_below, from_above, lane, r)[1]
                if r == 0:
                    part = from_low[8 * ex : 8 * (ex + 1), :]
                    move = (128 - 8 * j) % 128
                    part = pltpu.roll(part, move, 1) if move else part
                    x = x + jnp.where(lane % 64 < 8, part, 0.0)
                if r == EY - 1:
                    part = from_high[8 * ex : 8 * (ex + 1), :]
                    x = x + jnp.where(lane % 64 >= 56, pltpu.roll(part, 56 - 8 * j, 1), 0.0)
                out[rows : rows + 8, 128 * j : 128 * (j + 1)] = x


def in_vmem(array):
    return pltpu.with_memory_space_constraint(array, pltpu.VMEM)


def ring(array, count, shift):
    return lax.ppermute(array, "grp", [(i, (i + shift) % count) for i in range(count)])


def on_device(obs_coord, obs_resid, obs_weight, obs_dest, obs_send_slot, obs_elem, obs_slot):
    peer_count = lax.axis_size("dev")
    group_count = lax.axis_size("grp")
    row_count = obs_resid.shape[0]
    capacity = 2 * row_count // peer_count
    wide = min(256, capacity)
    per_peer = capacity // wide
    message_rows = -(-(FIELDS * per_peer + 1) // 8) * 8
    block = 2 * row_count
    lines = (FIELDS - 1) * PIECES + 1
    f32 = jnp.float32
    flat = [a.reshape(1, row_count) for a in (obs_resid, obs_weight, obs_dest, obs_send_slot, obs_elem)]
    send = pl.pallas_call(
        functools.partial(pack_kernel, capacity=capacity, wide=wide, chunk=row_count),
        out_shape=pltpu.VMEM((peer_count, message_rows, wide), f32),
        scratch_shapes=[pltpu.VMEM((lines * 2 * row_count // wide, wide), f32)],
        name="pack",
    )(obs_coord, *flat)
    got = lax.all_to_all(send, "dev", split_axis=0, concat_axis=0, tiled=True)
    plane = pltpu.VMEM((4 * EY + 8, 128), f32)
    field, to_below, to_above, part = pl.pallas_call(
        functools.partial(field_kernel, capacity=capacity, wide=wide, block=block),
        out_shape=(
            pltpu.VMEM((ELEM_DEV, 512), f32),
            plane,
            plane,
            pltpu.VMEM((8, 128), f32),
        ),
        scratch_shapes=[
            pltpu.VMEM((2 * 512, ELEM_DEV), f32),
            pltpu.VMEM((ELEM_DEV, 512), f32),
            pltpu.VMEM((ELEM_DEV, block), jnp.bfloat16),
            pltpu.VMEM((2 * 512, block), jnp.bfloat16),
        ],
        name="field",
    )(in_vmem(got))
    from_below, from_above = (
        in_vmem(ring(to_below_or_above, group_count, shift))
        for to_below_or_above, shift in ((to_above, 1), (to_below, group_count - 1))
    )
    others = [in_vmem(ring(part, group_count, group_count - k)) for k in range(2, group_count - 1)]
    field, part = in_vmem(field), in_vmem(part)
    edge = pltpu.VMEM((EX * EZ, 128), f32)
    to_low, to_high, cost = pl.pallas_call(
        edge_kernel,
        out_shape=(edge, edge, jax.ShapeDtypeStruct((1, 128), f32)),
        name="edge",
    )(field, from_below, from_above, part, *others)
    forward = [(i, i + 1) for i in range(peer_count - 1)]
    backward = [(target, source) for source, target in forward]
    from_low = lax.ppermute(to_high, "dev", forward)
    from_high = lax.ppermute(to_low, "dev", backward)
    nodal = pl.pallas_call(
        finish_kernel,
        out_shape=jax.ShapeDtypeStruct((ELEM_DEV, 512), f32),
        name="finish",
    )(field, from_below, from_above, in_vmem(from_low), in_vmem(from_high))
    return (nodal.reshape(EX, EY, EZ, 512), cost[0, 0])


def solution(mesh):
    placed = (
        P(None, ("grp", "dev")),
        P(("grp", "dev")),
        P(("grp", "dev")),
        P(("grp", "dev")),
        P(("grp", "dev")),
        P(("grp", "dev")),
        P(("grp", "dev")),
    )
    return jax.shard_map(
        on_device,
        mesh=mesh,
        in_specs=placed,
        out_specs=(P("grp", "dev", None, None), P()),
        check_vma=False,
    )
```

```python
import functools
import math

import jax
import jax.numpy as jnp
from jax import lax
from jax.experimental import pallas as pl
from jax.experimental.pallas import tpu as pltpu
from jax.sharding import PartitionSpec as P

EX = 4
EY = 8
EZ = 8
ELEM_DEV = 256
NODES = 8
FIELDS = 5
PIECES = 3
ANCHORS = [-math.cos(math.pi * k / 7) for k in range(NODES)]
SCALES = [
    1.0 / math.prod(ANCHORS[i] - ANCHORS[m] for m in range(NODES) if m != i) for i in range(NODES)
]
NT = (((1,), (1,)), ((), ()))


def pieces_of(values):
    first = values.astype(jnp.bfloat16)
    rest = values - first.astype(jnp.float32)
    second = rest.astype(jnp.bfloat16)
    third = rest - second.astype(jnp.float32)
    return [first.astype(jnp.float32), second.astype(jnp.float32), third]


def pack_kernel(coord, resid, weight, dest, slot, elem, out, acc, *, capacity, wide, chunk):
    rows = resid.shape[1]
    per_peer = capacity // wide
    high_count = 2 * rows // wide
    acc[...] = jnp.zeros_like(acc)
    lane_ids = lax.broadcasted_iota(jnp.int32, (wide, chunk), 0)
    high_ids = lax.broadcasted_iota(jnp.int32, (high_count, chunk), 0)

    def step(i, cost):
        at = pl.ds(pl.multiple_of(i * chunk, chunk), chunk)
        residual = resid[:, at]
        forcing = weight[:, at] * residual
        target = dest[:, at] * capacity + slot[:, at]
        high = target // wide
        low = target - high * wide
        right = jnp.where(lane_ids == low, 1.0, 0.0).astype(jnp.bfloat16)
        chosen = high_ids == high
        pieces = pieces_of(jnp.concatenate([coord[:, at], forcing], axis=0))
        lines = [piece[k : k + 1, :] for k in range(FIELDS - 1) for piece in pieces]
        lines.append(elem[:, at].astype(jnp.float32))
        left = jnp.concatenate(
            [
                jnp.where(chosen, jnp.broadcast_to(line, chosen.shape), 0.0).astype(jnp.bfloat16)
                for line in lines
            ],
            axis=0,
        )
        acc[...] += lax.dot_general(left, right, NT, preferred_element_type=jnp.float32)
        return cost + forcing * residual

    cost = lax.fori_loop(0, rows // chunk, step, jnp.zeros((1, chunk), jnp.float32))
    cost = 0.5 * jnp.sum(cost, axis=1, keepdims=True)
    used = FIELDS * per_peer
    for k in range(FIELDS):
        base = k * PIECES * high_count
        total = acc[base : base + high_count, :]
        for p in range(1, PIECES if k < FIELDS - 1 else 1):
            total = total + acc[base + p * high_count : base + (p + 1) * high_count, :]
        for peer in range(out.shape[0]):
            out[peer, k * per_peer : (k + 1) * per_peer, :] = total[
                peer * per_peer : (peer + 1) * per_peer, :
            ]
    for peer in range(out.shape[0]):
        out[peer, used:, :] = jnp.broadcast_to(cost, (out.shape[1] - used, wide))


def basis_of(position, node, scale):
    factor = scale
    for m in range(NODES):
        factor = factor * jnp.where(node == m, 1.0, position - ANCHORS[m])
    return factor


def field_kernel(got, field, to_below, to_above, cost, acc, raw, elems, outer, *, capacity, wide, block):
    peer_count = got.shape[0]
    per_peer = capacity // wide
    parts = block // wide
    node = lax.broadcasted_iota(jnp.int32, (NODES, wide), 0)
    scale = jnp.zeros((NODES, wide), jnp.float32)
    for i in range(NODES):
        scale = jnp.where(node == i, SCALES[i], scale)
    elem_ids = lax.broadcasted_iota(jnp.int32, (ELEM_DEV, wide), 0).astype(jnp.float32)
    elem_ids = elem_ids.astype(jnp.bfloat16)
    one = jnp.ones((ELEM_DEV, wide), jnp.bfloat16)
    acc[...] = jnp.zeros_like(acc)

    def step(i, carry):
        for q in range(parts):
            peer = i * (parts // per_peer) + q // per_peer
            row = q % per_peer
            u, v, w, f, e = (
                got[peer, row + k * per_peer : row + k * per_peer + 1, :] for k in range(FIELDS)
            )
            lanes = slice(q * wide, (q + 1) * wide)
            elems[:, lanes] = jnp.where(elem_ids == e.astype(jnp.bfloat16), one, jnp.zeros_like(one))
            first_w = basis_of(u, node, scale) * f
            second_w = basis_of(v, node, scale)
            third_w = basis_of(w, node, scale)
            inner = [second_w[b : b + 1, :] * third_w for b in range(NODES)]
            for a in range(NODES):
                mine = jnp.broadcast_to(first_w[a : a + 1, :], (NODES, wide))
                whole = jnp.concatenate([mine * inner[b] for b in range(NODES)], axis=0)
                head = whole.astype(jnp.bfloat16)
                rest = (whole - head.astype(jnp.float32)).astype(jnp.bfloat16)
                outer[64 * a : 64 * (a + 1), lanes] = head
                outer[512 + 64 * a : 512 + 64 * (a + 1), lanes] = rest
        acc[...] += lax.dot_general(
            outer[...], elems[...], NT, preferred_element_type=jnp.float32
        )
        return carry

    lax.fori_loop(0, peer_count * capacity // block, step, 0)
    raw[...] = (acc[:512] + acc[512:]).T

    lane = lax.broadcasted_iota(jnp.int32, (EZ, 128), 1)
    level = lax.broadcasted_iota(jnp.int32, (EZ, 128), 0)
    take_up = jnp.logical_and(lane % 8 == 7, level < EZ - 1)
    take_down = jnp.logical_and(lane % 8 == 0, level > 0)
    columns = []
    for j in range(4):
        blocks = []
        for r in range(EX * EY):
            x = raw[8 * r : 8 * (r + 1), 128 * j : 128 * (j + 1)]
            up = pltpu.roll(pltpu.roll(x, EZ - 1, 0), 7, 1)
            down = pltpu.roll(pltpu.roll(x, 1, 0), 121, 1)
            blocks.append(x + jnp.where(take_up, up, 0.0) + jnp.where(take_down, down, 0.0))
        column = []
        for r in range(EX * EY):
            x = blocks[r]
            if r % EY < EY - 1:
                x = x + jnp.where(lane % 64 >= 56, pltpu.roll(blocks[r + 1], 56, 1), 0.0)
            if r % EY > 0:
                x = x + jnp.where(lane % 64 < 8, pltpu.roll(blocks[r - 1], 72, 1), 0.0)
            column.append(x)
        if j in (1, 2):
            for r in range(EX * EY):
                field[8 * r : 8 * (r + 1), 128 * j : 128 * (j + 1)] = column[r]
        columns.append(column)
    lower, upper = columns[0], columns[3]
    for r in range(EX * EY):
        x, y = lower[r], upper[r]
        if r >= EY:
            x = x + jnp.where(lane < 64, pltpu.roll(upper[r - EY], 64, 1), 0.0)
        if r < (EX - 1) * EY:
            y = y + jnp.where(lane >= 64, pltpu.roll(lower[r + EY], 64, 1), 0.0)
        field[8 * r : 8 * (r + 1), 0:128] = x
        field[8 * r : 8 * (r + 1), 384:512] = y
    half = EY // 2
    used = FIELDS * per_peer
    total = got[0, used : used + 1, 0:128]
    for peer in range(1, peer_count):
        total = total + got[peer, used : used + 1, 0:128]
    total = jnp.broadcast_to(total, (8, 128))
    last = (EX - 1) * EY
    for r in range(half):
        to_below[8 * r : 8 * (r + 1), :] = jnp.where(
            lane < 64, lower[r], pltpu.roll(lower[r + half], 64, 1)
        )
        to_above[8 * r : 8 * (r + 1), :] = jnp.where(
            lane < 64, pltpu.roll(upper[last + r], 64, 1), upper[last + r + half]
        )
    to_below[8 * half :, :] = total
    to_above[8 * half :, :] = total
    cost[...] = total


def neighbours(from_below, from_above, lane, r):
    count = lax.axis_size("grp")
    half = EY // 2
    mine = lax.axis_index("grp")
    at = 8 * (r % half)
    low = from_below[at : at + 8, :]
    high = from_above[at : at + 8, :]
    if r >= half:
        low = pltpu.roll(low, 64, 1)
    else:
        high = pltpu.roll(high, 64, 1)
    low = jnp.where(jnp.logical_and(lane < 64, mine > 0), low, 0.0)
    high = jnp.where(jnp.logical_and(lane >= 64, mine < count - 1), high, 0.0)
    return low, high


def edge_kernel(field, from_below, from_above, *rest):
    *costs, to_low, to_high, cost = rest
    lane = lax.broadcasted_iota(jnp.int32, (EZ, 128), 1)
    for ex in range(EX):
        for r, out, shift in ((0, to_low, 0), (EY - 1, to_high, 72)):
            rows = 8 * (ex * EY + r)
            mask = lane % 64 >= 56 if shift else lane % 64 < 8
            total = jnp.zeros((EZ, 128), jnp.float32)
            for j in range(4):
                x = field[rows : rows + 8, 128 * j : 128 * (j + 1)]
                if ex == 0 and j == 0:
                    x = x + neighbours(from_below, from_above, lane, r)[0]
                if ex == EX - 1 and j == 3:
                    x = x + neighbours(from_below, from_above, lane, r)[1]
                x = jnp.where(mask, x, 0.0)
                move = (shift + 8 * j) % 128
                total = total + (pltpu.roll(x, move, 1) if move else x)
            out[8 * ex : 8 * (ex + 1), :] = total
    count = lax.axis_size("grp")
    mine = lax.axis_index("grp")
    row = slice(4 * EY, 4 * EY + 1)
    known = [costs[0][0:1, :], from_below[row, :], from_above[row, :]]
    known += [other[0:1, :] for other in costs[1:]]
    shifts = [0, count - 1, 1] + list(range(2, count - 1))
    total = jnp.zeros((1, 128), jnp.float32)
    for group in range(count):
        for shift, value in zip(shifts, known):
            total = total + jnp.where((mine + shift) % count == group, value, 0.0)
    cost[...] = total


def finish_kernel(field, from_below, from_above, from_low, from_high, out):
    lane = lax.broadcasted_iota(jnp.int32, (EZ, 128), 1)
    for ex in range(EX):
        for r in range(EY):
            rows = 8 * (ex * EY + r)
            for j in range(4):
                x = field[rows : rows + 8, 128 * j : 128 * (j + 1)]
                if ex == 0 and j == 0:
                    x = x + neighbours(from_below, from_above, lane, r)[0]
                if ex == EX - 1 and j == 3:
                    x = x + neighbours(from_below, from_above, lane, r)[1]
                if r == 0:
                    part = from_low[8 * ex : 8 * (ex + 1), :]
                    move = (128 - 8 * j) % 128
                    part = pltpu.roll(part, move, 1) if move else part
                    x = x + jnp.where(lane % 64 < 8, part, 0.0)
                if r == EY - 1:
                    part = from_high[8 * ex : 8 * (ex + 1), :]
                    x = x + jnp.where(lane % 64 >= 56, pltpu.roll(part, 56 - 8 * j, 1), 0.0)
                out[rows : rows + 8, 128 * j : 128 * (j + 1)] = x


def in_vmem(array):
    return pltpu.with_memory_space_constraint(array, pltpu.VMEM)


def ring(array, count, shift):
    return lax.ppermute(array, "grp", [(i, (i + shift) % count) for i in range(count)])


def on_device(obs_coord, obs_resid, obs_weight, obs_dest, obs_send_slot, obs_elem, obs_slot):
    peer_count = lax.axis_size("dev")
    group_count = lax.axis_size("grp")
    row_count = obs_resid.shape[0]
    capacity = 2 * row_count // peer_count
    wide = min(256, capacity)
    per_peer = capacity // wide
    message_rows = -(-(FIELDS * per_peer + 1) // 8) * 8
    block = 2 * row_count
    lines = (FIELDS - 1) * PIECES + 1
    f32 = jnp.float32
    flat = [a.reshape(1, row_count) for a in (obs_resid, obs_weight, obs_dest, obs_send_slot, obs_elem)]
    send = pl.pallas_call(
        functools.partial(pack_kernel, capacity=capacity, wide=wide, chunk=row_count),
        out_shape=pltpu.VMEM((peer_count, message_rows, wide), f32),
        scratch_shapes=[pltpu.VMEM((lines * 2 * row_count // wide, wide), f32)],
        name="pack",
    )(obs_coord, *flat)
    got = lax.all_to_all(send, "dev", split_axis=0, concat_axis=0, tiled=True)
    plane = pltpu.VMEM((4 * EY + 8, 128), f32)
    field, to_below, to_above, part = pl.pallas_call(
        functools.partial(field_kernel, capacity=capacity, wide=wide, block=block),
        out_shape=(
            pltpu.VMEM((ELEM_DEV, 512), f32),
            plane,
            plane,
            pltpu.VMEM((8, 128), f32),
        ),
        scratch_shapes=[
            pltpu.VMEM((2 * 512, ELEM_DEV), f32),
            pltpu.VMEM((ELEM_DEV, 512), f32),
            pltpu.VMEM((ELEM_DEV, block), jnp.bfloat16),
            pltpu.VMEM((2 * 512, block), jnp.bfloat16),
        ],
        name="field",
    )(in_vmem(got))
    from_below, from_above = (
        in_vmem(ring(to_below_or_above, group_count, shift))
        for to_below_or_above, shift in ((to_above, 1), (to_below, group_count - 1))
    )
    others = [in_vmem(ring(part, group_count, group_count - k)) for k in range(2, group_count - 1)]
    field, part = in_vmem(field), in_vmem(part)
    edge = pltpu.VMEM((EX * EZ, 128), f32)
    to_low, to_high, cost = pl.pallas_call(
        edge_kernel,
        out_shape=(edge, edge, jax.ShapeDtypeStruct((1, 128), f32)),
        name="edge",
    )(field, from_below, from_above, part, *others)
    forward = [(i, i + 1) for i in range(peer_count - 1)]
    backward = [(target, source) for source, target in forward]
    from_low = lax.ppermute(to_high, "dev", forward)
    from_high = lax.ppermute(to_low, "dev", backward)
    nodal = pl.pallas_call(
        finish_kernel,
        out_shape=jax.ShapeDtypeStruct((ELEM_DEV, 512), f32),
        name="finish",
    )(field, from_below, from_above, in_vmem(from_low), in_vmem(from_high))
    return (nodal.reshape(EX, EY, EZ, 512), cost[0, 0])


def solution(mesh):
    placed = (
        P(None, ("grp", "dev")),
        P(("grp", "dev")),
        P(("grp", "dev")),
        P(("grp", "dev")),
        P(("grp", "dev")),
        P(("grp", "dev")),
        P(("grp", "dev")),
    )
    return jax.shard_map(
        on_device,
        mesh=mesh,
        in_specs=placed,
        out_specs=(P("grp", "dev", None, None), P()),
        check_vma=False,
    )
```
